32 devices in a mesh: parts: 2 (over y), blk: 4 (over z), sub: 2 (over x), rep: 2 (over core).
Axes of the slice: x: 2, y: 2, z: 4, core: 2. Of those that a mesh axis runs over, the one named last changes fastest.
Arguments:
- queries: bfloat16 [128, 32, 128], P(('parts', 'blk', 'sub', 'rep')), parts along dimension 0, may hold values from -1.5 to 1.5
- passages: bfloat16 [512, 128, 128], P(('parts', 'blk')), parts along dimension 0, may hold values from -1.5 to 1.5
- lengths: int32 [512], P(('parts', 'blk')), parts along dimension 0, may hold values from 8 to 128
- slot_of: int32 [512], P('parts'), parts along dimension 0, may hold values from 0 to 255, each once
- candidates: int32 [128, 256], P(('parts', 'blk', 'sub', 'rep')), parts along dimension 0, may hold values from 0 to 255
Outputs:
- score: float32 [128, 256], P(('parts', 'blk', 'sub', 'rep')), parts along dimension 0
- top: float32 [128, 10], P(('parts', 'blk', 'sub', 'rep')), parts along dimension 0
The draws below stay inside these ranges and needn't reach their ends.
There are 2 independent parts, one for each index of `parts`. The reference program is written for one: setup_inputs(seed, part) draws one part's arguments, and reference() takes and returns one part's arrays. A program takes and returns all parts, laid end to end along the dimension named above; each array names one. Nothing has to cross between parts.
Inputs may be any that keep to these rules, and one draw needn't show every extreme that they name: `slot_of`: a permutation; storage row r lies on the blk index r // 64. `candidates`: passage ids, repeats allowed. `lengths`: the live slots of a row are its first ones.
All inputs are finite; a program needn't handle non-finite values.
Results may differ from the reference program's by a relative error of at most 0.0003.
Values may be sent and summed in bfloat16 or wider, within the bound.
No kernel may reach another device: no remote copies, remote signals or barrier semaphores. Data moves between devices by JAX's collectives and lax.ppermute only.
A program may use at most 64 MiB of HBM per device.

```python
import math
import jax
import jax.numpy as jnp
import numpy as np
from jax import lax

DIM = 128
QT = 32
LP = 128
K = 256
TOPN = 10
NQ = 64
NP = 256


def set_ends(drawn, stream_key, low, high):
    extent = drawn.shape
    index_at = [jax.random.randint(jax.random.fold_in(stream_key, axis), (), 0, extent[axis]) for axis in range(len(extent))]
    drawn = drawn.at[tuple(index_at)].set(low)
    longest = extent.index(max(extent))
    index_at[longest] = (index_at[longest] + 1) % extent[longest]
    return drawn.at[tuple(index_at)].set(high)


def steps_of(own_key, extent, split, least, high):
    loudness, own = 1.0, jax.random.fold_in(own_key, 6)
    for axis_at, shards_of in split:
        heights = jnp.exp(jax.random.uniform(jax.random.fold_in(own, axis_at), (shards_of,), jnp.float32, least / len(split), high / len(split)))
        loudness = loudness * jnp.repeat(heights, extent[axis_at] // shards_of).reshape([-1 if axis == axis_at else 1 for axis in range(len(extent))])
    return loudness


def cumulative_ranks(count, skew):
    loads = [(1 << 20) // math.isqrt(grade ** skew) + 1 for grade in range(1, count + 1)]
    scale = 1 + sum(loads) // (1 << 30)
    return np.cumsum(np.array([max(1, weight // scale) for weight in loads]))


def skewed_ids(own_key, extent, number_of, lean):
    grid = cumulative_ranks(number_of, lean)
    ticket = jax.random.randint(jax.random.fold_in(own_key, 1), extent, 0, int(grid[number_of - 1]))
    grade = jnp.searchsorted(jnp.asarray(grid, jnp.int32), ticket, side="right")
    return jax.random.permutation(jax.random.fold_in(own_key, 2), number_of)[grade].astype(jnp.int32)


def noise(key, extent, scale, bound, pieces=(), kind=jnp.bfloat16):
    entries = jax.random.normal(key, extent, jnp.float32) * scale
    if len(pieces) > 0:
        entries = steps_of(key, extent, pieces, -0.22, 0.18) * entries
    return jnp.clip(entries, min=-bound, max=bound).astype(kind)


def setup_inputs(seed: int = 0, part: int = 0) -> dict:
    key_of = jax.random.split(jax.random.key(seed), 6)
    part_splits = jax.random.split(jax.random.fold_in(key_of[5], part), 6)
    return {
        "queries": noise(part_splits[0], (NQ, QT, DIM), 0.25, 1.5, ((0, 16),)),
        "passages": noise(part_splits[1], (NP, LP, DIM), 0.25, 1.5, ((0, 4),)),
        "lengths": set_ends(jax.random.randint(part_splits[2], (NP,), 8, LP + 1), jax.random.fold_in(part_splits[2], 1), 8, LP).astype(jnp.int32),
        "slot_of": jax.random.permutation(part_splits[3], NP).astype(jnp.int32),
        "candidates": set_ends(skewed_ids(part_splits[4], (NQ, K), NP, 2), jax.random.fold_in(part_splits[4], 3), 0, NP - 1).astype(jnp.int32),
    }


def reference(queries, passages, lengths, slot_of, candidates):
    query_count = queries.shape[0]
    passage_count = passages.shape[0]
    flat = queries.reshape(query_count * QT, DIM)
    blocks = passages.reshape(passage_count // 8, 8 * LP, DIM)
    spans = lengths.reshape(passage_count // 8, 8)

    def one_block(pair):
        piece, live_count = pair
        similar = jnp.dot(flat, piece.T, preferred_element_type=jnp.float32)
        similar = similar.reshape(query_count * QT, 8, LP)
        live = jnp.arange(LP, dtype=jnp.int32)[None, :] < live_count[:, None]
        best = jnp.max(jnp.where(live[None], similar, -1e30), axis=2)
        return jnp.sum(best.reshape(query_count, QT, 8), axis=1) / QT

    table = lax.map(one_block, (blocks, spans))
    table = jnp.transpose(table, (1, 0, 2)).reshape(query_count, passage_count)
    storage_rows = jnp.take(slot_of, candidates, axis=0).astype(jnp.int32)
    score = jnp.take_along_axis(table, storage_rows, axis=1)
    top = lax.top_k(score, TOPN)[0]
    return score, top
```

```python
import functools

import jax
import jax.numpy as jnp
from jax import lax
from jax.experimental import pallas as pl
from jax.experimental.pallas import tpu as pltpu
from jax.sharding import PartitionSpec as P

TOPN = 10
LANES = 128
SUBLANES = 8
LEAST = -1e30
UNITS = 2


def spread(tokens):
    blank = jnp.zeros_like(tokens)
    return jnp.concatenate(
        [jnp.concatenate([tokens, blank], axis=1), jnp.concatenate([blank, tokens], axis=1)], axis=0
    )


def token_best(accs, passages, limits, tokens):
    count, span, _ = passages.shape
    width = tokens.shape[0]
    pairs = count // 2
    slots = len(accs) // UNITS
    rhs = spread(tokens)
    for unit in range(UNITS):
        pltpu.matmul_push_rhs(rhs, staging_register=0, mxu_index=unit, transpose=True)
    slot = lax.broadcasted_iota(jnp.int32, (span, width), 0)
    tops, waiting = [[], []], []

    def drain():
        pair, acc = waiting.pop(0)
        similar = pltpu.matmul_pop(acc)
        for half in range(2):
            index = pair + half * pairs
            live = slot < limits[index : index + 1, :]
            kept = jnp.where(live, similar[:, half * width : (half + 1) * width], LEAST)
            tops[half].append(jnp.max(kept.reshape(span // SUBLANES, SUBLANES, width), axis=0))

    for pair in range(pairs):
        acc = accs[pair % UNITS * slots + pair // UNITS % slots]
        lhs = jnp.concatenate([passages[pair], passages[pair + pairs]], axis=1)
        pltpu.matmul_acc_lhs(acc, lhs, load_staged_rhs=0 if pair < UNITS else None)
        waiting.append((pair, acc))
        if len(waiting) > len(accs) // 2:
            drain()
    while waiting:
        drain()
    group = min(SUBLANES, pairs)
    ordered = tops[0] + tops[1]
    return jnp.concatenate(
        [jnp.max(jnp.stack(ordered[start : start + group]), axis=1) for start in range(0, count, group)], axis=0
    )


def accumulators(span):
    slots = 4 * 256 // span
    return [pltpu.ACC(unit)((span, 256), jnp.float32) for unit in range(UNITS) for _ in range(slots)]


def scores_of(best, queries_here):
    turned = best.T
    tokens = turned.shape[0] // queries_here
    return jnp.sum(turned.reshape(queries_here, tokens, turned.shape[1]), axis=1) / tokens


def lookup(table, index):
    low = index % LANES
    high = index // LANES
    out = jnp.zeros(index.shape, table.dtype)
    for part in range(table.shape[1] // LANES):
        piece = table[:, part * LANES : (part + 1) * LANES]
        found = jnp.take_along_axis(piece, low, axis=1)
        out = jnp.where(high == part, found, out)
    return out


def lookup_wide(table, index):
    return jnp.concatenate(
        [
            lookup(table, index[:, start : start + LANES])
            for start in range(0, index.shape[1], LANES)
        ],
        axis=1,
    )


def own_kernel(lengths, queries, passages, slots, candidates, table, limits, rows, *, queries_here, owners):
    count, span, width = passages.shape
    for index in range(count):
        limits[index : index + 1, :] = jnp.full((1, limits.shape[1]), lengths[index], jnp.int32)
    row = slots[...]
    step = (row // count + (owners - lax.axis_index("blk"))) % owners
    relative = step * count + row % count
    wanted = candidates[...]
    wanted = jnp.concatenate([wanted] * (SUBLANES // queries_here), axis=0)
    rows[...] = lookup_wide(jnp.broadcast_to(relative, (SUBLANES, row.shape[1])), wanted)

    def body(*accs):
        table[...] = scores_of(token_best(accs, passages, limits, queries[...]), queries_here)

    pl.run_scoped(body, *accumulators(span))


def arrived_kernel(queries, passages, limits, table, *, queries_here):
    def body(*accs):
        table[...] = scores_of(token_best(accs, passages, limits, queries[...]), queries_here)

    pl.run_scoped(body, *accumulators(passages.shape[1]))


def finish_kernel(rows, *refs):
    pieces = refs[:-2]
    score, top = refs[-2:]
    queries_here = score.shape[0]
    table = jnp.concatenate([piece[...] for piece in pieces], axis=1)
    table = jnp.concatenate([table] * (SUBLANES // queries_here), axis=0)
    found = lookup_wide(table, rows[...])
    score[...] = found[:queries_here]
    lane = lax.broadcasted_iota(jnp.int32, (SUBLANES, LANES), 1)
    ranked = jnp.zeros((SUBLANES, LANES), jnp.float32)
    taken = jnp.zeros((SUBLANES, 1), jnp.int32)
    for _ in range(TOPN):
        largest = jnp.max(found, axis=1, keepdims=True)
        same = found == largest
        ranked = jnp.where(lane >= taken, largest, ranked)
        taken = taken + jnp.sum(same.astype(jnp.int32), axis=1, keepdims=True)
        found = jnp.where(same, -jnp.inf, found)
    top[...] = ranked[:queries_here, :TOPN]


def near(value):
    return pltpu.with_memory_space_constraint(value, pltpu.VMEM)


def whole(memory=pltpu.VMEM):
    return pl.BlockSpec(memory_space=memory)


def shards(queries, passages, lengths, slot_of, candidates, owners):
    queries_here, tokens, width = queries.shape
    count, span, _ = passages.shape
    flat = queries.reshape(queries_here * tokens, width)
    ids = slot_of.shape[0]
    wanted = candidates.shape[1]

    def shift(value, step):
        pairs = [(index, (index + step) % owners) for index in range(owners)]
        return lax.ppermute(value, "blk", pairs)

    arrived = [shift(flat, step) for step in range(1, owners)]
    flops = 2 * flat.shape[0] * count * span * width
    estimate = pl.CostEstimate(flops=flops, bytes_accessed=2 * passages.size, transcendentals=0)
    piece_shape = pltpu.VMEM((queries_here, count), jnp.float32)
    stored = near(passages)
    own, limits, rows = pl.pallas_call(
        functools.partial(own_kernel, queries_here=queries_here, owners=owners),
        out_shape=(
            piece_shape,
            pltpu.VMEM((count, flat.shape[0]), jnp.int32),
            pltpu.VMEM((SUBLANES, wanted), jnp.int32),
        ),
        in_specs=[whole(pltpu.SMEM), whole(), whole(), whole(), whole()],
        out_specs=(whole(), whole(), whole()),
        cost_estimate=estimate,
        name="own",
    )(lengths, near(flat), stored, near(slot_of.reshape(1, ids)), near(candidates))
    pieces = [own]
    for step in range(1, owners):
        piece = pl.pallas_call(
            functools.partial(arrived_kernel, queries_here=queries_here),
            out_shape=piece_shape,
            in_specs=[whole(), whole(), whole()],
            out_specs=whole(),
            cost_estimate=estimate,
            name="arrived",
        )(near(arrived[step - 1]), stored, near(limits))
        pieces.append(shift(piece, owners - step))
    score, top = pl.pallas_call(
        finish_kernel,
        out_shape=(
            jax.ShapeDtypeStruct((queries_here, wanted), jnp.float32),
            jax.ShapeDtypeStruct((queries_here, TOPN), jnp.float32),
        ),
        in_specs=[whole()] * (1 + owners),
        out_specs=(whole(), whole()),
        name="finish",
    )(near(rows), *[near(piece) for piece in pieces])
    return score, top


def solution(mesh):
    return jax.shard_map(
        functools.partial(shards, owners=mesh.shape["blk"]),
        mesh=mesh,
        in_specs=(
            P(("parts", "blk", "sub", "rep"), None, None),
            P(("parts", "blk"), None, None),
            P(("parts", "blk")),
            P("parts"),
            P(("parts", "blk", "sub", "rep"), None),
        ),
        out_specs=(
            P(("parts", "blk", "sub", "rep"), None),
            P(("parts", "blk", "sub", "rep"), None),
        ),
        check_vma=False,
    )
```
